32 devices in a mesh: owner: 4 (over x, core), rows: 8 (over z, y).
Axes of the slice: x: 2, y: 2, z: 4, core: 2. Of those that a mesh axis runs over, the one named last changes fastest.
Arguments:
- master_down: float32 [8, 14336, 4096], P('owner', None, 'rows'), may hold values from -0.046875 to 0.046875
- router_weight: float32 [4096, 8], P('rows', 'owner'), may hold values from -0.09375 to 0.09375
- router_gain: float32 [4096], P('rows'), may hold values from 0.25 to 1.75
Outputs:
- final_down: bfloat16 [8, 4096, 14336], P('owner', None, 'rows')
- serve_router: bfloat16 [4096, 8], replicated
The draws below stay inside these ranges and needn't reach their ends.
All inputs are finite; a program needn't handle non-finite values.
Results may differ from the reference program's by a relative error of at most 0.001.
Values may be sent and summed in bfloat16 or wider, within the bound.
No kernel may reach another device: no remote copies, remote signals or barrier semaphores. Data moves between devices by JAX's collectives and lax.ppermute only.
A program may use at most 192 MiB of HBM per device.

```python
import jax
import jax.numpy as jnp

EXPERTS = 8
D_MODEL = 4096
D_EXPERT = 14336


def steps_of(key, extent, split, smallest, largest):
    def one(axis_at, parts):
        heights = jax.random.uniform(jax.random.fold_in(jax.random.fold_in(key, 6), axis_at), (parts,), jnp.float32, smallest / len(split), largest / len(split))
        return jnp.repeat(jnp.exp(heights), extent[axis_at] // parts).reshape((-1,) + (1,) * (len(extent) - axis_at - 1))

    gain = one(*split[0])
    for cut in split[1:]:
        gain = gain * one(*cut)
    return gain


def noise(own_key, dims, width, reach, pieces=(), dtype=jnp.bfloat16):
    level = steps_of(own_key, dims, pieces, -0.22, 0.18) if pieces else 1.0
    result = jax.random.normal(own_key, dims, jnp.float32) * width * level
    return jnp.minimum(jnp.maximum(result, -reach), reach).astype(dtype)


def setup_inputs(seed: int = 0) -> dict:
    streams_of = jax.random.split(jax.random.key(seed), 4)
    master_down = noise(streams_of[0], (EXPERTS, D_EXPERT, D_MODEL), D_EXPERT ** -0.5, 0.046875, ((0, 4), (2, 8)), jnp.float32)
    router_weight = noise(streams_of[1], (D_MODEL, EXPERTS), D_MODEL ** -0.5, 0.09375, ((0, 8), (1, 4)), jnp.float32)
    router_gain = jnp.clip(1.0 + 0.15 * jax.random.normal(streams_of[2], (D_MODEL,), jnp.float32), 0.25, 1.75)
    return dict(master_down=master_down, router_weight=router_weight, router_gain=router_gain)


def reference(master_down, router_weight, router_gain):
    final_down = master_down.astype(jnp.bfloat16)
    final_down = jnp.transpose(final_down, (0, 2, 1))
    serve_router = (router_weight * router_gain[:, None]).astype(jnp.bfloat16)
    return final_down, serve_router
```

```python
import functools

import jax
import jax.numpy as jnp
from jax import lax
from jax.experimental import pallas as pl
from jax.experimental.pallas import tpu as pltpu
from jax.sharding import PartitionSpec as P


def turn_body(where, full, after, piece):
    del where, after
    piece[0] = full[0].astype(jnp.bfloat16).T


def turn(where, full, after, expert, height, name):
    columns = full.shape[2]
    step = min(columns, 128)
    return pl.pallas_call(
        turn_body,
        grid_spec=pltpu.PrefetchScalarGridSpec(
            num_scalar_prefetch=1,
            grid=(columns // step,),
            in_specs=[
                pl.BlockSpec((1, height, step), lambda c, where: (expert, where[0], c)),
                pl.BlockSpec(memory_space=pl.ANY),
            ],
            out_specs=pl.BlockSpec((1, step, height), lambda c, where: (0, c, 0)),
        ),
        out_shape=jax.ShapeDtypeStruct((1, columns, height), jnp.bfloat16),
        compiler_params=pltpu.CompilerParams(dimension_semantics=("arbitrary",)),
        name=name,
    )(where, full, after)


def keep_body(where, full, whole):
    del where
    whole[0] = full[0].astype(jnp.bfloat16).T


def keep(where, full, parts, height):
    experts, _, columns = full.shape
    step = min(columns, 128)
    blocks = columns // step
    return pl.pallas_call(
        keep_body,
        grid_spec=pltpu.PrefetchScalarGridSpec(
            num_scalar_prefetch=1,
            grid=(experts, blocks),
            in_specs=[pl.BlockSpec((1, height, step), lambda e, c, where: (e, where[0], c))],
            out_specs=pl.BlockSpec((1, step, height), lambda e, c, where: (e, where[0] * blocks + c, 0)),
        ),
        out_shape=jax.ShapeDtypeStruct((experts, columns * parts, height), jnp.bfloat16),
        compiler_params=pltpu.CompilerParams(dimension_semantics=("arbitrary", "arbitrary")),
        name="keep",
    )(where, full)


def put_body(where, piece, old, whole):
    del where, old
    whole[...] = piece[...]


def put(where, piece, whole, expert, name):
    _, columns, height = piece.shape
    step = min(columns, 128)
    blocks = columns // step
    return pl.pallas_call(
        put_body,
        grid_spec=pltpu.PrefetchScalarGridSpec(
            num_scalar_prefetch=1,
            grid=(blocks,),
            in_specs=[
                pl.BlockSpec((1, step, height), lambda c, where: (0, c, 0)),
                pl.BlockSpec(memory_space=pl.ANY),
            ],
            out_specs=pl.BlockSpec((1, step, height), lambda c, where: (expert, where[0] * blocks + c, 0)),
        ),
        out_shape=jax.ShapeDtypeStruct(whole.shape, whole.dtype),
        input_output_aliases={2: 0},
        compiler_params=pltpu.CompilerParams(dimension_semantics=("arbitrary",)),
        name=name,
    )(where, piece, whole)


def order_of(parts, experts):
    far = [(k, e) for e in range(experts) for k in range(parts // 2, parts)]
    near = [(k, e) for e in range(experts) for k in range(parts // 2 - 1, 0, -1)]
    order = []
    while far or near:
        if far:
            order.append(far.pop(0))
        if near:
            order.append(near.pop(0))
    return order


def shards(master_down, router_weight, router_gain):
    parts = lax.axis_size("rows")
    me = lax.axis_index("rows")
    experts, inner, columns = master_down.shape
    height = inner // parts

    def pairs(k):
        return [(d, d ^ k) for d in range(parts)]

    def place(k):
        return (me ^ k).astype(jnp.int32).reshape(1)

    order = order_of(parts, experts)
    after = router_gain
    got = []
    for k, e in order:
        after = turn(place(k), master_down, after, e, height, f"turn_{k}_{e}")
        got.append(lax.ppermute(after, "rows", pairs(k)))

    own_router = (router_weight * router_gain[:, None]).astype(jnp.bfloat16).T
    wide_router = lax.all_gather(own_router, "owner", axis=0, tiled=True)
    routers = [wide_router]
    for k in range(1, parts):
        routers.append(lax.ppermute(wide_router, "rows", pairs(k)))

    final_down = keep(place(0), master_down, parts, height)
    for (k, e), piece in zip(order, got):
        final_down = put(place(k), piece, final_down, e, f"put_{k}_{e}")

    stack = jnp.stack(routers)
    bit = 1
    while bit < parts:
        split = stack.reshape((parts // (2 * bit), 2, bit) + wide_router.shape)
        swapped = jnp.where((me & bit) != 0, split[:, ::-1], split)
        stack = swapped.reshape(stack.shape)
        bit *= 2
    serve_router = jnp.transpose(stack, (0, 2, 1)).reshape(-1, wide_router.shape[0])
    return (final_down, serve_router)


def solution(mesh):
    return jax.shard_map(
        shards,
        mesh=mesh,
        in_specs=(P("owner", None, "rows"), P("rows", "owner"), P("rows")),
        out_specs=(P("owner", None, "rows"), P()),
        check_vma=False,
    )
```

```python
import jax
import jax.numpy as jnp
from jax import lax
from jax.experimental import pallas as pl
from jax.experimental.pallas import tpu as pltpu
from jax.sharding import PartitionSpec as P

ANY = pl.BlockSpec(memory_space=pl.ANY)


def rows_of(height):
    return 256 if height % 256 == 0 else height


def turn(full, after, piece, height, name):
    k, expert, start, width = piece
    rows = rows_of(height)
    count = height // rows

    def body(full, after, out, wide, narrow, come, go):
        del after
        first = (lax.axis_index("rows") ^ k) * height
        ins, outs = [], []
        for i in range(count):
            source = full.at[expert, pl.ds(pl.multiple_of(first + i * rows, 64), rows), pl.ds(start, width)]
            ins.append(pltpu.make_async_copy(source, wide.at[i], come.at[i]))
            part = pl.ds(i * rows, rows)
            outs.append(pltpu.make_async_copy(narrow.at[:, part], out.at[0, :, part], go.at[i]))
        for copy in ins:
            copy.start()
        for i in range(count):
            ins[i].wait()
            narrow[:, i * rows : (i + 1) * rows] = wide[i].astype(jnp.bfloat16).T
            outs[i].start()
        for copy in outs:
            copy.wait()

    return pl.pallas_call(
        body,
        in_specs=[ANY, ANY],
        out_specs=ANY,
        out_shape=jax.ShapeDtypeStruct((1, width, height), jnp.bfloat16),
        scratch_shapes=[
            pltpu.VMEM((count, rows, width), jnp.float32),
            pltpu.VMEM((width, height), jnp.bfloat16),
            pltpu.SemaphoreType.DMA((count,)),
            pltpu.SemaphoreType.DMA((count,)),
        ],
        name=name,
    )(full, after)


def keep_body(where, full, after, whole):
    del where, after
    whole[0] = full[0].astype(jnp.bfloat16).T


def keep(where, full, after, parts, height):
    experts, _, columns = full.shape
    step = min(columns, 128)
    blocks = columns // step
    return pl.pallas_call(
        keep_body,
        grid_spec=pltpu.PrefetchScalarGridSpec(
            num_scalar_prefetch=1,
            grid=(experts, blocks),
            in_specs=[pl.BlockSpec((1, height, step), lambda e, c, where: (e, where[0], c)), ANY],
            out_specs=pl.BlockSpec((1, step, height), lambda e, c, where: (e, where[0] * blocks + c, 0)),
        ),
        out_shape=jax.ShapeDtypeStruct((experts, columns * parts, height), jnp.bfloat16),
        compiler_params=pltpu.CompilerParams(dimension_semantics=("arbitrary", "arbitrary")),
        name="keep",
    )(where, full, after)


def put(got, whole, piece, columns, name):
    k, expert, start, width = piece
    height = whole.shape[2]
    step = min(width, 128)
    count = width // step

    def body(got, old, whole, held, come, go):
        del old
        first = (lax.axis_index("rows") ^ k) * columns + start
        ins, outs = [], []
        for i in range(count):
            ins.append(pltpu.make_async_copy(got.at[0, pl.ds(i * step, step)], held.at[i], come.at[i]))
            target = whole.at[expert, pl.ds(pl.multiple_of(first + i * step, step), step)]
            outs.append(pltpu.make_async_copy(held.at[i], target, go.at[i]))
        for copy in ins:
            copy.start()
        for i in range(count):
            ins[i].wait()
            outs[i].start()
        for copy in outs:
            copy.wait()

    return pl.pallas_call(
        body,
        in_specs=[ANY, ANY],
        out_specs=ANY,
        out_shape=jax.ShapeDtypeStruct(whole.shape, whole.dtype),
        input_output_aliases={1: 0},
        scratch_shapes=[
            pltpu.VMEM((count, step, height), whole.dtype),
            pltpu.SemaphoreType.DMA((count,)),
            pltpu.SemaphoreType.DMA((count,)),
        ],
        name=name,
    )(got, whole)


def fold_body(weight, gain, after, out):
    del after
    out[...] = (weight[...] * gain[...]).astype(jnp.bfloat16)


def fold(weight, gain, after):
    return pl.pallas_call(
        fold_body,
        in_specs=[pl.BlockSpec(memory_space=pltpu.VMEM), pl.BlockSpec(memory_space=pltpu.VMEM), ANY],
        out_specs=pl.BlockSpec(memory_space=pltpu.VMEM),
        out_shape=jax.ShapeDtypeStruct(weight.shape, jnp.bfloat16),
        name="fold",
    )(weight, gain, after)


def order_of(parts, experts, columns):
    step = min(columns, 128)
    far = [(k, e, 0, columns) for e in range(experts) for k in range(parts // 2, parts)]
    near = [(k, e, 0, columns) for e in range(experts) for k in range(parts // 2 - 1, 0, -1)]
    if step < columns:
        k, e, _, _ = far[0]
        far[:1] = [(k, e, 0, step), (k, e, step, columns - step)]
        k, e, _, _ = far[-1]
        far[-1:] = [(k, e, 0, columns - step), (k, e, columns - step, step)]
    order = [far.pop(0)]
    while far or near:
        if far:
            order.append(far.pop(0))
        if near:
            order.append(near.pop(0))
    return order


def shards(master_down, router_weight, router_gain):
    parts = lax.axis_size("rows")
    me = lax.axis_index("rows")
    experts, inner, columns = master_down.shape
    height = inner // parts

    def pairs(k):
        return [(d, d ^ k) for d in range(parts)]

    order = order_of(parts, experts, columns)
    after = router_gain
    got, turned = [], []
    for i, piece in enumerate(order):
        after = turn(master_down, after, piece, height, f"turn_{i}")
        turned.append(after)
        got.append(lax.ppermute(after, "rows", pairs(piece[0])))

    own_router = fold(router_weight.T, router_gain[None, :], turned[min(4, len(turned) - 1)])
    wide_router = lax.all_gather(own_router, "owner", axis=0, tiled=True)
    routers = [wide_router]
    for k in range(1, parts):
        routers.append(lax.ppermute(wide_router, "rows", pairs(k)))

    final_down = keep(me.astype(jnp.int32).reshape(1), master_down, after, parts, height)
    for i, piece in enumerate(order):
        final_down = put(got[i], final_down, piece, columns, f"put_{i}")

    stack = jnp.stack(routers)
    bit = 1
    while bit < parts:
        split = stack.reshape((parts // (2 * bit), 2, bit) + wide_router.shape)
        swapped = jnp.where((me & bit) != 0, split[:, ::-1], split)
        stack = swapped.reshape(stack.shape)
        bit *= 2
    serve_router = jnp.transpose(stack, (0, 2, 1)).reshape(-1, wide_router.shape[0])
    return (final_down, serve_router)


def solution(mesh):
    return jax.shard_map(
        shards,
        mesh=mesh,
        in_specs=(P("owner", None, "rows"), P("rows", "owner"), P("rows")),
        out_specs=(P("owner", None, "rows"), P()),
        check_vma=False,
    )
```

```python
import jax
import jax.numpy as jnp
from jax import lax
from jax.experimental import pallas as pl
from jax.experimental.pallas import tpu as pltpu
from jax.sharding import PartitionSpec as P

ANY = pl.BlockSpec(memory_space=pl.ANY)


def cuts_of(rows):
    step = 256 if rows % 128 == 0 else rows
    return [(at, min(step, rows - at)) for at in range(0, rows, step)]


def turn(full, after, piece, height, name):
    k, expert, start, rows = piece
    columns = full.shape[2]
    cuts = cuts_of(rows)

    def body(full, after, out, wide, narrow, come, go):
        del after
        first = (lax.axis_index("rows") ^ k) * height + start
        ins, outs = [], []
        for i, (at, size) in enumerate(cuts):
            part = pl.ds(at, size)
            source = full.at[expert, pl.ds(pl.multiple_of(first + at, 64), size)]
            ins.append(pltpu.make_async_copy(source, wide.at[part], come.at[i]))
            outs.append(pltpu.make_async_copy(narrow.at[:, part], out.at[0, :, part], go.at[i]))
        for copy in ins:
            copy.start()
        for i, (at, size) in enumerate(cuts):
            ins[i].wait()
            narrow[:, at : at + size] = wide[at : at + size].astype(jnp.bfloat16).T
            outs[i].start()
        for copy in outs:
            copy.wait()

    return pl.pallas_call(
        body,
        in_specs=[ANY, ANY],
        out_specs=ANY,
        out_shape=jax.ShapeDtypeStruct((1, columns, rows), jnp.bfloat16),
        scratch_shapes=[
            pltpu.VMEM((rows, columns), jnp.float32),
            pltpu.VMEM((columns, rows), jnp.bfloat16),
            pltpu.SemaphoreType.DMA((len(cuts),)),
            pltpu.SemaphoreType.DMA((len(cuts),)),
        ],
        name=name,
    )(full, after)


def keep_body(where, full, after, whole):
    del where, after
    whole[0] = full[0].astype(jnp.bfloat16).T


def keep(where, full, after, parts, height):
    experts, _, columns = full.shape
    step = min(columns, 128)
    blocks = columns // step
    return pl.pallas_call(
        keep_body,
        grid_spec=pltpu.PrefetchScalarGridSpec(
            num_scalar_prefetch=1,
            grid=(experts, blocks),
            in_specs=[pl.BlockSpec((1, height, step), lambda e, c, where: (e, where[0], c)), ANY],
            out_specs=pl.BlockSpec((1, step, height), lambda e, c, where: (e, where[0] * blocks + c, 0)),
        ),
        out_shape=jax.ShapeDtypeStruct((experts, columns * parts, height), jnp.bfloat16),
        compiler_params=pltpu.CompilerParams(dimension_semantics=("arbitrary", "arbitrary")),
        name="keep",
    )(where, full, after)


def put(got, whole, after, piece, name):
    k, expert, start, rows = piece
    columns = got.shape[1]
    step = min(columns, 128)
    count = columns // step

    def body(got, old, after, whole, held, come, go):
        del old, after
        first = (lax.axis_index("rows") ^ k) * columns
        ins, outs = [], []
        for i in range(count):
            ins.append(pltpu.make_async_copy(got.at[0, pl.ds(i * step, step)], held.at[i], come.at[i]))
            target = whole.at[expert, pl.ds(pl.multiple_of(first + i * step, step), step), pl.ds(start, rows)]
            outs.append(pltpu.make_async_copy(held.at[i], target, go.at[i]))
        for copy in ins:
            copy.start()
        for i in range(count):
            ins[i].wait()
            outs[i].start()
        for copy in outs:
            copy.wait()

    return pl.pallas_call(
        body,
        in_specs=[ANY, ANY, ANY],
        out_specs=ANY,
        out_shape=jax.ShapeDtypeStruct(whole.shape, whole.dtype),
        input_output_aliases={1: 0},
        scratch_shapes=[
            pltpu.VMEM((count, step, rows), whole.dtype),
            pltpu.SemaphoreType.DMA((count,)),
            pltpu.SemaphoreType.DMA((count,)),
        ],
        name=name,
    )(got, whole, after)


def fold_body(weight, gain, after, out):
    del after
    out[...] = (weight[...] * gain[...]).astype(jnp.bfloat16)


def fold(weight, gain, after):
    return pl.pallas_call(
        fold_body,
        in_specs=[pl.BlockSpec(memory_space=pltpu.VMEM), pl.BlockSpec(memory_space=pltpu.VMEM), ANY],
        out_specs=pl.BlockSpec(memory_space=pltpu.VMEM),
        out_shape=jax.ShapeDtypeStruct(weight.shape, jnp.bfloat16),
        name="fold",
    )(weight, gain, after)


def order_of(parts, experts, height):
    lead = max(parts - 2, parts // 2)
    others = [k for k in range(parts // 2, parts) if k != lead]
    far = [(k, e, 0, height) for e in range(experts) for k in ([lead] + others if e < experts - 1 else others + [lead])]
    near = [(k, e, 0, height) for e in range(experts) for k in range(parts // 2 - 1, 0, -1)]
    if height % 128 == 0 and height > 256:
        far[:1] = [(lead, far[0][1], 0, 256), (lead, far[0][1], 256, height - 256)]
        far[-1:] = [(lead, far[-1][1], 0, height - 128), (lead, far[-1][1], height - 128, 128)]
    order = [far.pop(0)]
    while far or near:
        if far:
            order.append(far.pop(0))
        if near:
            order.append(near.pop(0))
    return order


def shards(master_down, router_weight, router_gain):
    parts = lax.axis_size("rows")
    me = lax.axis_index("rows")
    experts, inner, _ = master_down.shape
    height = inner // parts

    def pairs(k):
        return [(d, d ^ k) for d in range(parts)]

    order = order_of(parts, experts, height)
    after = router_gain
    got, turned = [], []
    for i, piece in enumerate(order):
        after = turn(master_down, after, piece, height, f"turn_{i}")
        turned.append(after)
        got.append(lax.ppermute(after, "rows", pairs(piece[0])))

    own_router = fold(router_weight.T, router_gain[None, :], turned[min(4, len(turned) - 1)])
    stack = jnp.stack([own_router] + [lax.ppermute(own_router, "rows", pairs(k)) for k in range(1, parts)])
    bit = 1
    while bit < parts:
        split = stack.reshape((parts // (2 * bit), 2, bit) + own_router.shape)
        swapped = jnp.where((me & bit) != 0, split[:, ::-1], split)
        stack = swapped.reshape(stack.shape)
        bit *= 2
    high_router = jnp.transpose(stack, (1, 0, 2)).reshape(own_router.shape[0], -1)
    serve_router = lax.all_gather(high_router, "owner", axis=0, tiled=True)

    final_down = keep(me.astype(jnp.int32).reshape(1), master_down, after, parts, height)
    for i, piece in enumerate(order):
        ready = serve_router if i == len(order) // 2 else router_gain
        final_down = put(got[i], final_down, ready, piece, f"put_{i}")
    return (final_down, serve_router.T)


def solution(mesh):
    return jax.shard_map(
        shards,
        mesh=mesh,
        in_specs=(P("owner", None, "rows"), P("rows", "owner"), P("rows")),
        out_specs=(P("owner", None, "rows"), P()),
        check_vma=False,
    )
```

```python
import jax
import jax.numpy as jnp
from jax import lax
from jax.experimental import pallas as pl
from jax.experimental.pallas import tpu as pltpu
from jax.sharding import PartitionSpec as P

ANY = pl.BlockSpec(memory_space=pl.ANY)


def turn(full, after, piece, height, name):
    k, expert, start, rows = piece
    columns = full.shape[2]

    def body(full, after, out, wide, narrow, come, go):
        del after
        first = (lax.axis_index("rows") ^ k) * height + start
        source = full.at[expert, pl.ds(pl.multiple_of(first, 64), rows)]
        copy = pltpu.make_async_copy(source, wide, come)
        copy.start()
        copy.wait()
        narrow[...] = wide[...].astype(jnp.bfloat16).T
        copy = pltpu.make_async_copy(narrow, out.at[0], go)
        copy.start()
        copy.wait()

    return pl.pallas_call(
        body,
        in_specs=[ANY, ANY],
        out_specs=ANY,
        out_shape=jax.ShapeDtypeStruct((1, columns, rows), jnp.bfloat16),
        scratch_shapes=[
            pltpu.VMEM((rows, columns), jnp.float32),
            pltpu.VMEM((columns, rows), jnp.bfloat16),
            pltpu.SemaphoreType.DMA,
            pltpu.SemaphoreType.DMA,
        ],
        name=name,
    )(full, after)


def keep_body(where, full, after, whole):
    del where, after
    whole[0] = full[0].astype(jnp.bfloat16).T


def keep(where, full, after, parts, height):
    experts, _, columns = full.shape
    step = columns
    blocks = 1
    return pl.pallas_call(
        keep_body,
        grid_spec=pltpu.PrefetchScalarGridSpec(
            num_scalar_prefetch=1,
            grid=(experts, blocks),
            in_specs=[pl.BlockSpec((1, height, step), lambda e, c, where: (e, where[0], c)), ANY],
            out_specs=pl.BlockSpec((1, step, height), lambda e, c, where: (e, where[0] * blocks + c, 0)),
        ),
        out_shape=jax.ShapeDtypeStruct((experts, columns * parts, height), jnp.bfloat16),
        compiler_params=pltpu.CompilerParams(dimension_semantics=("arbitrary", "arbitrary")),
        name="keep",
    )(where, full, after)


def put(got, whole, after, piece, name):
    k, expert, start, rows = piece
    columns = got.shape[1]
    step = min(columns, 128) if rows == 128 else columns
    count = columns // step

    def body(got, old, after, whole, held, come, go):
        del old, after
        first = (lax.axis_index("rows") ^ k) * columns
        ins, outs = [], []
        for i in range(count):
            ins.append(pltpu.make_async_copy(got.at[0, pl.ds(i * step, step)], held.at[i], come.at[i]))
            target = whole.at[expert, pl.ds(pl.multiple_of(first + i * step, step), step), pl.ds(start, rows)]
            outs.append(pltpu.make_async_copy(held.at[i], target, go.at[i]))
        for copy in ins:
            copy.start()
        for i in range(count):
            ins[i].wait()
            outs[i].start()
        for copy in outs:
            copy.wait()

    return pl.pallas_call(
        body,
        in_specs=[ANY, ANY, ANY],
        out_specs=ANY,
        out_shape=jax.ShapeDtypeStruct(whole.shape, whole.dtype),
        input_output_aliases={1: 0},
        scratch_shapes=[
            pltpu.VMEM((count, step, rows), whole.dtype),
            pltpu.SemaphoreType.DMA((count,)),
            pltpu.SemaphoreType.DMA((count,)),
        ],
        name=name,
    )(got, whole, after)


def fold_body(weight, gain, after, out):
    del after
    out[...] = (weight[...] * gain[...]).astype(jnp.bfloat16)


def fold(weight, gain, after):
    return pl.pallas_call(
        fold_body,
        in_specs=[pl.BlockSpec(memory_space=pltpu.VMEM), pl.BlockSpec(memory_space=pltpu.VMEM), ANY],
        out_specs=pl.BlockSpec(memory_space=pltpu.VMEM),
        out_shape=jax.ShapeDtypeStruct(weight.shape, jnp.bfloat16),
        name="fold",
    )(weight, gain, after)


def order_of(parts, experts, height):
    lead = max(parts - 2, parts // 2)
    others = [k for k in range(parts // 2, parts) if k != lead]
    far = [(k, e, 0, height) for e in range(experts) for k in ([lead] + others if e < experts - 1 else others + [lead])]
    near = [(k, e, 0, height) for e in range(experts) for k in range(parts // 2 - 1, 0, -1)]
    if height % 128 == 0 and height > 256:
        far[:1] = [(lead, far[0][1], 0, 256), (lead, far[0][1], 256, height - 256)]
        far[-1:] = [(lead, far[-1][1], 0, height - 128), (lead, far[-1][1], height - 128, 128)]
    order = [far.pop(0)]
    while far or near:
        if far:
            order.append(far.pop(0))
        if near:
            order.append(near.pop(0))
    return order


def shards(master_down, router_weight, router_gain):
    parts = lax.axis_size("rows")
    me = lax.axis_index("rows")
    experts, inner, _ = master_down.shape
    height = inner // parts

    def pairs(k):
        return [(d, d ^ k) for d in range(parts)]

    order = order_of(parts, experts, height)
    after = router_gain
    got, turned = [], []
    for i, piece in enumerate(order):
        after = turn(master_down, after, piece, height, f"turn_{i}")
        turned.append(after)
        got.append(lax.ppermute(after, "rows", pairs(piece[0])))

    own_router = fold(router_weight.T, router_gain[None, :], turned[min(4, len(turned) - 1)])
    stack = jnp.stack([own_router] + [lax.ppermute(own_router, "rows", pairs(k)) for k in range(1, parts)])
    bit = 1
    while bit < parts:
        split = stack.reshape((parts // (2 * bit), 2, bit) + own_router.shape)
        swapped = jnp.where((me & bit) != 0, split[:, ::-1], split)
        stack = swapped.reshape(stack.shape)
        bit *= 2
    high_router = jnp.transpose(stack, (1, 0, 2)).reshape(own_router.shape[0], -1)
    serve_router = lax.all_gather(high_router, "owner", axis=0, tiled=True)

    final_down = keep(me.astype(jnp.int32).reshape(1), master_down, after, parts, height)
    for i, piece in enumerate(order):
        ready = serve_router if i == len(order) // 2 else router_gain
        final_down = put(got[i], final_down, ready, piece, f"put_{i}")
    return (final_down, serve_router.T)


def solution(mesh):
    return jax.shard_map(
        shards,
        mesh=mesh,
        in_specs=(P("owner", None, "rows"), P("rows", "owner"), P("rows")),
        out_specs=(P("owner", None, "rows"), P()),
        check_vma=False,
    )
```

```python
import jax
import jax.numpy as jnp
from jax import lax
from jax.experimental import pallas as pl
from jax.experimental.pallas import tpu as pltpu
from jax.sharding import PartitionSpec as P


ANY = pl.BlockSpec(memory_space=pl.ANY)


def cuts_of(rows):
    step = min(256, rows // 2 if rows % 256 == 0 else rows) if rows % 128 == 0 else rows
    return [(at, min(step, rows - at)) for at in range(0, rows, step)]


def turn(full, after, piece, height):
    k, expert, start, rows = piece
    columns = full.shape[2]
    cuts = cuts_of(rows)

    def body(full, after, out, wide, narrow, come, go):
        del after
        first = (lax.axis_index("rows") ^ k) * height + start
        ins, outs = [], []
        for i, (at, size) in enumerate(cuts):
            part = pl.ds(at, size)
            source = full.at[expert, pl.ds(pl.multiple_of(first + at, 64), size)]
            ins.append(pltpu.make_async_copy(source, wide.at[part], come.at[i]))
            outs.append(pltpu.make_async_copy(narrow.at[:, part], out.at[0, :, part], go.at[i]))
        for copy in ins:
            copy.start()
        for i, (at, size) in enumerate(cuts):
            ins[i].wait()
            narrow[:, at : at + size] = wide[at : at + size].astype(jnp.bfloat16).T
            outs[i].start()
        for copy in outs:
            copy.wait()

    return pl.pallas_call(
        body,
        in_specs=[ANY, ANY],
        out_specs=ANY,
        out_shape=jax.ShapeDtypeStruct((1, columns, rows), jnp.bfloat16),
        scratch_shapes=[
            pltpu.VMEM((rows, columns), jnp.float32),
            pltpu.VMEM((columns, rows), jnp.bfloat16),
            pltpu.SemaphoreType.DMA((len(cuts),)),
            pltpu.SemaphoreType.DMA((len(cuts),)),
        ],
    )(full, after)


def keep_body(where, full, after, whole):
    del where, after
    whole[0] = full[0].astype(jnp.bfloat16).T


def keep(where, full, after, parts, height):
    experts, _, columns = full.shape
    step = min(columns, 128)
    blocks = columns // step
    return pl.pallas_call(
        keep_body,
        grid_spec=pltpu.PrefetchScalarGridSpec(
            num_scalar_prefetch=1,
            grid=(experts, blocks),
            in_specs=[pl.BlockSpec((1, height, step), lambda e, c, where: (e, where[0], c)), ANY],
            out_specs=pl.BlockSpec((1, step, height), lambda e, c, where: (e, where[0] * blocks + c, 0)),
        ),
        out_shape=jax.ShapeDtypeStruct((experts, columns * parts, height), jnp.bfloat16),
        compiler_params=pltpu.CompilerParams(dimension_semantics=("arbitrary", "arbitrary")),
        name="keep",
    )(where, full, after)


def put(got, whole, after, piece):
    k, expert, start, rows = piece
    columns = got.shape[1]
    step = min(columns, 128)
    count = columns // step

    def body(got, old, after, whole, held, come, go):
        del old, after
        first = (lax.axis_index("rows") ^ k) * columns
        ins, outs = [], []
        for i in range(count):
            ins.append(pltpu.make_async_copy(got.at[0, pl.ds(i * step, step)], held.at[i], come.at[i]))
            target = whole.at[expert, pl.ds(pl.multiple_of(first + i * step, step), step), pl.ds(start, rows)]
            outs.append(pltpu.make_async_copy(held.at[i], target, go.at[i]))
        for copy in ins:
            copy.start()
        for i in range(count):
            ins[i].wait()
            outs[i].start()
        for copy in outs:
            copy.wait()

    return pl.pallas_call(
        body,
        in_specs=[ANY, ANY, ANY],
        out_specs=ANY,
        out_shape=jax.ShapeDtypeStruct(whole.shape, whole.dtype),
        input_output_aliases={1: 0},
        scratch_shapes=[
            pltpu.VMEM((count, step, rows), whole.dtype),
            pltpu.SemaphoreType.DMA((count,)),
            pltpu.SemaphoreType.DMA((count,)),
        ],
    )(got, whole, after)


def fold_body(weight, gain, after, out):
    del after
    out[...] = (weight[...] * gain[...]).astype(jnp.bfloat16)


def fold(weight, gain, after):
    return pl.pallas_call(
        fold_body,
        in_specs=[pl.BlockSpec(memory_space=pltpu.VMEM), pl.BlockSpec(memory_space=pltpu.VMEM), ANY],
        out_specs=pl.BlockSpec(memory_space=pltpu.VMEM),
        out_shape=jax.ShapeDtypeStruct(weight.shape, jnp.bfloat16),
        name="fold",
    )(weight, gain, after)


def order_of(parts, experts, height):
    lead = max(parts - 2, parts // 2)
    others = [k for k in range(parts // 2, parts) if k != lead]
    far = [(k, e, 0, height) for e in range(experts) for k in ([lead] + others if e < experts - 1 else others + [lead])]
    near = [(k, e, 0, height) for e in range(experts) for k in range(parts // 2 - 1, 0, -1)]
    if height % 128 == 0 and height > 256:
        far[:1] = [(lead, far[0][1], 0, 256), (lead, far[0][1], 256, height - 256)]
        far[-1:] = [(lead, far[-1][1], 0, height - 128), (lead, far[-1][1], height - 128, 128)]
    order = [far.pop(0)]
    while far or near:
        if far:
            order.append(far.pop(0))
        if near:
            order.append(near.pop(0))
    return order


def exchange(master_down, router_weight, router_gain):
    parts = lax.axis_size("rows")
    me = lax.axis_index("rows")
    experts, inner, _ = master_down.shape
    height = inner // parts

    def pairs(k):
        return [(d, d ^ k) for d in range(parts)]

    order = order_of(parts, experts, height)
    after = router_gain
    got, turned = [], []
    for piece in order:
        after = turn(master_down, after, piece, height)
        turned.append(after)
        got.append(lax.ppermute(after, "rows", pairs(piece[0])))

    own_router = fold(router_weight.T, router_gain[None, :], turned[min(1, len(turned) - 1)])
    half = parts // 2
    far_router = lax.ppermute(own_router, "rows", pairs(half))
    both = jnp.stack([own_router, far_router])
    stack = jnp.concatenate([both] + [lax.ppermute(both, "rows", pairs(k)) for k in range(1, half)])
    stack = jnp.swapaxes(stack.reshape((half, 2) + own_router.shape), 0, 1).reshape((parts,) + own_router.shape)
    bit = 1
    while bit < parts:
        split = stack.reshape((parts // (2 * bit), 2, bit) + own_router.shape)
        swapped = jnp.where((me & bit) != 0, split[:, ::-1], split)
        stack = swapped.reshape(stack.shape)
        bit *= 2
    high_router = jnp.transpose(stack, (1, 0, 2)).reshape(own_router.shape[0], -1)
    serve_router = lax.all_gather(high_router, "owner", axis=0, tiled=True)

    final_down = keep(me.astype(jnp.int32).reshape(1), master_down, after, parts, height)
    for i, piece in enumerate(order):
        ready = serve_router if i == len(order) // 2 else router_gain
        final_down = put(got[i], final_down, ready, piece)
    return (final_down, serve_router.T)


def solution(mesh):
    return jax.shard_map(
        exchange,
        mesh=mesh,
        in_specs=(P("owner", None, "rows"), P("rows", "owner"), P("rows")),
        out_specs=(P("owner", None, "rows"), P()),
        check_vma=False,
    )
```
